32 devices in a mesh: row: 16 (over z, y, core), col: 2 (over x).
Axes of the slice: x: 2, y: 2, z: 4, core: 2. Of those that a mesh axis runs over, the one named last changes fastest.
Arguments:
- pair_rep: bfloat16 [2048, 2048, 128], P('row', 'col'), may hold values from -6 to 6
- bias_weight: bfloat16 [128, 12], replicated, may hold values from -0.5 to 0.5
- head_weight: float32 [12], replicated, may hold values from -1 to 1
- queries: float32 [192, 2048], P(None, 'row'), may hold values from -48 to 48, as said below
- key_vectors: float32 [192, 2048], P(None, 'col'), may hold values from -48 to 48, as said below
- values: float32 [192, 2048], P(None, 'col'), may hold values from -6 to 6
- query_points: float32 [3, 48, 2048], P(None, None, 'row'), may hold values from -6 to 6
- key_points: float32 [3, 48, 2048], P(None, None, 'col'), may hold values from -6 to 6
- value_points: float32 [3, 96, 2048], P(None, None, 'col'), may hold values from -6 to 6
- rotations: float32 [3, 3, 2048], replicated, may hold values from -1 to 1, as said below
- translations: float32 [3, 2048], replicated, may hold values from -12 to 12
- residue_count: int32 [1], replicated, may hold values from 1024 to 2048
- grad_output: float32 [192, 2048], P(None, 'row'), may hold values from -6 to 6
- grad_points: float32 [3, 96, 2048], P(None, None, 'row'), may hold values from -6 to 6
- grad_pair: bfloat16 [2048, 12, 128], P('row'), may hold values from -2 to 2
Outputs:
- pair_grad: bfloat16 [2048, 2048, 128], P('row', 'col')
- query_grad: float32 [192, 2048], P(None, ('row', 'col'))
- query_point_grad: float32 [3, 48, 2048], P(None, None, ('row', 'col'))
- query_frame_grad: float32 [3, 4, 2048], P(None, None, ('row', 'col'))
- key_grad: float32 [192, 2048], P(None, ('col', 'row'))
- value_grad: float32 [192, 2048], P(None, ('col', 'row'))
- key_point_grad: float32 [3, 48, 2048], P(None, None, ('col', 'row'))
- value_point_grad: float32 [3, 96, 2048], P(None, None, ('col', 'row'))
- key_frame_grad: float32 [3, 4, 2048], P(None, None, ('col', 'row'))
- bias_weight_grad: float32 [128, 12], replicated
- head_weight_grad: float32 [12], replicated
The draws below stay inside these ranges and needn't reach their ends.
Inputs may be any that keep to these rules, and one draw needn't show every extreme that they name: `queries`: entries of order one, except a few residues whose vectors are much larger. `key_vectors`: entries of order one, except a few residues whose vectors are much larger. `rotations`: each residue's 3 x 3 matrix is a rotation: orthonormal with determinant one.
All inputs are finite; a program needn't handle non-finite values.
Results may differ from the reference program's by a relative error of at most 0.0049.
Values sent between devices are 32-bit elements; how exact they have to be, the bound alone decides.
A program may use at most 256 MiB of HBM per device.

```python
import math
import jax
import jax.numpy as jnp
from jax import lax

N = 2048
H = 12
C = 16
PQ = 4
PV = 8
CZ = 128


def drawn_vectors(key):
    base_key = jax.random.fold_in(key, 11)
    first, second = jax.random.split(base_key, 2)
    query_draw = jnp.clip(jax.random.normal(first, (H * C, N), jnp.float32), -4.0, 4.0)
    key_draw = jnp.clip(jax.random.normal(second, (H * C, N), jnp.float32), -4.0, 4.0)
    return (query_draw, key_draw)


def draw_queries(key, part):
    return drawn_vectors(key)[0]


def draw_key_vectors(key, part):
    return drawn_vectors(key)[1]


def draw_rotations(key, part):
    base_key = jax.random.fold_in(key, 23)
    first, second = jax.random.split(base_key)
    scalar = jax.random.uniform(first, (N,), jnp.float32, 0.5, 1.5)
    vector = jax.random.normal(second, (3, N), jnp.float32)
    length = jnp.sqrt(scalar ** 2 + jnp.sum(vector ** 2, axis=0))
    qw = scalar / length
    qx = vector[0] / length
    qy = vector[1] / length
    qz = vector[2] / length
    first_row = jnp.stack([1 - 2 * (qy * qy + qz * qz), 2 * (qx * qy - qw * qz), 2 * (qx * qz + qw * qy)])
    second_row = jnp.stack([2 * (qx * qy + qw * qz), 1 - 2 * (qx * qx + qz * qz), 2 * (qy * qz - qw * qx)])
    third_row = jnp.stack([2 * (qx * qz - qw * qy), 2 * (qy * qz + qw * qx), 1 - 2 * (qx * qx + qy * qy)])
    return jnp.stack([first_row, second_row, third_row])


def levels(stream_key, dims, shards, least, high):
    factor_of, own = 1.0, jax.random.fold_in(stream_key, 6)
    for position, parts in shards:
        heights = jnp.exp(jax.random.uniform(jax.random.fold_in(own, position), (parts,), jnp.float32, least / len(shards), high / len(shards)))
        factor_of = factor_of * jnp.repeat(heights, dims[position] // parts).reshape([-1 if axis == position else 1 for axis in range(len(dims))])
    return factor_of


def gaussian(own_key, shape, deviation, most, pieces=(), kind=jnp.bfloat16):
    loudness = levels(own_key, shape, pieces, -0.22, 0.18) if pieces else 1.0
    drawn = jax.random.normal(own_key, shape, jnp.float32) * deviation * loudness
    return jnp.minimum(jnp.maximum(drawn, -most), most).astype(kind)


def setup_inputs(seed: int = 0) -> dict:
    key_list = jax.random.split(jax.random.key(seed), 16)
    return {
        "pair_rep": gaussian(key_list[0], (N, N, CZ), 1.0, 6.0, ((0, 16), (1, 2))),
        "bias_weight": gaussian(key_list[1], (CZ, H), CZ ** -0.5, 0.5),
        "head_weight": jnp.clip(jax.random.uniform(key_list[2], (H,), jnp.float32, -1.0, 1.0), -1.0, 1.0),
        "queries": draw_queries(jax.random.fold_in(key_list[15], 71), 0),
        "key_vectors": draw_key_vectors(jax.random.fold_in(key_list[15], 71), 0),
        "values": gaussian(key_list[5], (H * C, N), 1.0, 6.0, ((1, 2),), jnp.float32),
        "query_points": gaussian(key_list[6], (3, H * PQ, N), 1.0, 6.0, ((2, 16),), jnp.float32),
        "key_points": gaussian(key_list[7], (3, H * PQ, N), 1.0, 6.0, ((2, 2),), jnp.float32),
        "value_points": gaussian(key_list[8], (3, H * PV, N), 1.0, 6.0, ((2, 2),), jnp.float32),
        "rotations": draw_rotations(jax.random.fold_in(key_list[15], 71), 0),
        "translations": gaussian(key_list[10], (3, N), 2.0, 12.0, (), jnp.float32),
        "residue_count": jax.random.randint(key_list[11], (1,), N // 2, N + 1).astype(jnp.int32),
        "grad_output": gaussian(key_list[12], (H * C, N), 1.0, 6.0, ((1, 16),), jnp.float32),
        "grad_points": gaussian(key_list[13], (3, H * PV, N), 1.0, 6.0, ((2, 16),), jnp.float32),
        "grad_pair": gaussian(key_list[14], (N, H, CZ), 0.3, 2.0, ((0, 16),)),
    }


HIGHEST = lax.Precision.HIGHEST

def globalize(rotation, offset, local):
    return jnp.einsum('xym,ykm->xkm', rotation, local, precision=HIGHEST) + offset[:, None, :]

def rotate_back(rotation, vector):
    return jnp.einsum('xym,xkm->ykm', rotation, vector, precision=HIGHEST)

def frame_terms(grad_global, local):
    rotation_part = jnp.einsum('xkm,ykm->xym', grad_global, local, precision=HIGHEST)
    return jnp.concatenate([rotation_part, lax.optimization_barrier(jnp.sum(grad_global, axis=1))[:, None, :]], axis=1)

def output_frame_terms(point_out, offset, cotan_local, grad_rotated):
    rotation_part = jnp.einsum('xkm,ykm->xym', point_out - offset[:, None, :], cotan_local, precision=HIGHEST)
    return jnp.concatenate([rotation_part, -lax.optimization_barrier(jnp.sum(grad_rotated, axis=1))[:, None, :]], axis=1)

def reference(pair_rep, bias_weight, head_weight, queries, key_vectors, values, query_points, key_points, value_points, rotations, translations, residue_count, grad_output, grad_points, grad_pair):
    logit_scale = math.sqrt(1.0 / 3.0)
    point_scale = math.sqrt(2.0 / (9.0 * PQ))
    inner_scale = 1.0 / math.sqrt(C)
    distance_coef = 0.5 * logit_scale * point_scale * jax.nn.softplus(head_weight)
    query_global = globalize(rotations, translations, query_points).reshape(3, H, PQ, N)
    key_global = globalize(rotations, translations, key_points).reshape(3, H, PQ, N)
    value_global = globalize(rotations, translations, value_points).reshape(3, H, PV, N)
    grad_global = jnp.einsum('xym,ykm->xkm', rotations, grad_points, precision=HIGHEST)
    grad_heads = grad_global.reshape(3, H, PV, N)
    key_heads = key_vectors.reshape(H, C, N)
    value_heads = values.reshape(H, C, N)
    query_heads = queries.reshape(H, C, N)
    out_heads = grad_output.reshape(H, C, N)
    valid = jnp.arange(N) < residue_count[0]
    pair_weight = bias_weight.astype(jnp.float32)
    block = min(128, N)

    def step(carry, start):
        pair_block = lax.dynamic_slice_in_dim(pair_rep, start, block, 0).astype(jnp.float32)
        cotan_pair = lax.dynamic_slice_in_dim(grad_pair, start, block, 0).astype(jnp.float32)
        query_block = lax.dynamic_slice_in_dim(query_heads, start, block, 2)
        out_block = lax.dynamic_slice_in_dim(out_heads, start, block, 2)
        qglobal_block = lax.dynamic_slice_in_dim(query_global, start, block, 3)
        gglobal_block = lax.dynamic_slice_in_dim(grad_heads, start, block, 3)
        inner = jnp.einsum('hci,hcj->hij', query_block, key_heads, precision=HIGHEST)
        cross = jnp.einsum('xhpi,xhpj->hij', qglobal_block, key_global, precision=HIGHEST)
        distance = lax.optimization_barrier(jnp.sum(qglobal_block ** 2, axis=(0, 2)))[:, :, None] + lax.optimization_barrier(jnp.sum(key_global ** 2, axis=(0, 2)))[:, None, :] - 2.0 * cross
        bias = jnp.einsum('ijc,ch->hij', pair_block, pair_weight, precision=HIGHEST)
        logits = logit_scale * (inner_scale * inner + bias) - distance_coef[:, None, None] * distance
        logits = jnp.where(valid[None, None, :], logits, jnp.float32(-1000000000.0))
        row_peak = lax.optimization_barrier(jnp.max(logits, axis=2, keepdims=True))
        exponent = jnp.exp(logits - row_peak)
        attention = exponent / lax.optimization_barrier(jnp.sum(exponent, axis=2, keepdims=True))
        product = jnp.einsum('hci,hcj->hij', out_block, value_heads, precision=HIGHEST) + jnp.einsum('xhvi,xhvj->hij', gglobal_block, value_global, precision=HIGHEST) + jnp.einsum('ijc,ihc->hij', pair_block, cotan_pair, precision=HIGHEST)
        delta = lax.optimization_barrier(jnp.sum(attention * product, axis=2, keepdims=True))
        logit_grad = attention * (product - delta)
        query_grad = logit_scale * inner_scale * jnp.einsum('hij,hcj->hci', logit_grad, key_heads, precision=HIGHEST)
        row_sum = lax.optimization_barrier(jnp.sum(logit_grad, axis=2))
        qpoint_grad = -2.0 * distance_coef[None, :, None, None] * (qglobal_block * row_sum[None, :, None, :] - jnp.einsum('hij,xhpj->xhpi', logit_grad, key_global, precision=HIGHEST))
        qpoint_flat = qpoint_grad.reshape(3, H * PQ, block)
        point_out = jnp.einsum('hij,xhvj->xhvi', attention, value_global, precision=HIGHEST).reshape(3, H * PV, block)
        rot_block = lax.dynamic_slice_in_dim(rotations, start, block, 2)
        shift_block = lax.dynamic_slice_in_dim(translations, start, block, 1)
        local_block = lax.dynamic_slice_in_dim(query_points, start, block, 2)
        cotan_local = lax.dynamic_slice_in_dim(grad_points, start, block, 2)
        gflat_block = gglobal_block.reshape(3, H * PV, block)
        qlocal_grad = rotate_back(rot_block, qpoint_flat)
        qframe = frame_terms(qpoint_flat, local_block) + output_frame_terms(point_out, shift_block, cotan_local, gflat_block)
        key_part = logit_scale * inner_scale * jnp.einsum('hij,hci->hcj', logit_grad, query_block, precision=HIGHEST)
        value_part = jnp.einsum('hij,hci->hcj', attention, out_block, precision=HIGHEST)
        col_sum = lax.optimization_barrier(jnp.sum(logit_grad, axis=1))
        kpoint_part = 2.0 * distance_coef[None, :, None, None] * (jnp.einsum('hij,xhpi->xhpj', logit_grad, qglobal_block, precision=HIGHEST) - key_global * col_sum[None, :, None, :])
        vpoint_part = jnp.einsum('hij,xhvi->xhvj', attention, gglobal_block, precision=HIGHEST)
        grad_rounded = lax.optimization_barrier(logit_grad.astype(jnp.bfloat16)).astype(jnp.float32)
        attn_rounded = lax.optimization_barrier(attention.astype(jnp.bfloat16)).astype(jnp.float32)
        weight_part = logit_scale * jnp.einsum('ijc,hij->ch', pair_block, grad_rounded, precision=HIGHEST)
        distance_part = lax.optimization_barrier(jnp.sum(logit_grad * distance, axis=(1, 2)))
        pair_grad = (logit_scale * jnp.einsum('hij,ch->ijc', grad_rounded, pair_weight, precision=HIGHEST) + jnp.einsum('hij,ihc->ijc', attn_rounded, cotan_pair, precision=HIGHEST)).astype(jnp.bfloat16)
        new_carry = (carry[0] + key_part, carry[1] + value_part, carry[2] + kpoint_part, carry[3] + vpoint_part, carry[4] + weight_part, carry[5] + distance_part)
        return (new_carry, (pair_grad, query_grad.reshape(H * C, block), qlocal_grad, qframe))
    initial = (jnp.zeros((H, C, N), jnp.float32), jnp.zeros((H, C, N), jnp.float32), jnp.zeros((3, H, PQ, N), jnp.float32), jnp.zeros((3, H, PV, N), jnp.float32), jnp.zeros((CZ, H), jnp.float32), jnp.zeros((H,), jnp.float32))
    starts = jnp.arange(N // block, dtype=jnp.int32) * block
    carry, stacked = lax.scan(step, initial, starts)
    pair_grad = stacked[0].reshape(N, N, CZ)
    query_grad = jnp.transpose(stacked[1], (1, 0, 2)).reshape(H * C, N)
    query_point_grad = jnp.transpose(stacked[2], (1, 2, 0, 3)).reshape(3, H * PQ, N)
    query_frame_grad = jnp.transpose(stacked[3], (1, 2, 0, 3)).reshape(3, 4, N)
    kpoint_flat = carry[2].reshape(3, H * PQ, N)
    vpoint_flat = carry[3].reshape(3, H * PV, N)
    key_point_grad = rotate_back(rotations, kpoint_flat)
    value_point_grad = rotate_back(rotations, vpoint_flat)
    key_frame_grad = frame_terms(kpoint_flat, key_points) + frame_terms(vpoint_flat, value_points)
    head_weight_grad = carry[5] * (-0.5 * logit_scale * point_scale) * jax.nn.sigmoid(head_weight)
    return (pair_grad, query_grad, query_point_grad, query_frame_grad, carry[0].reshape(H * C, N), carry[1].reshape(H * C, N), key_point_grad, value_point_grad, key_frame_grad, carry[4], head_weight_grad)
```

```python
import functools
import math

import jax
import jax.numpy as jnp
from jax import lax
from jax.experimental import pallas as pl
from jax.experimental.pallas import tpu as pltpu
from jax.sharding import PartitionSpec as P

F32 = jnp.float32
BF16 = jnp.bfloat16
PAD = 16
VMEM_LIMIT = 60 * 1024 * 1024


def dot(a, b, dims):
    return lax.dot_general(a, b, (dims, ((), ())), preferred_element_type=F32)


TN = ((0,), (0,))
NT = ((1,), (1,))
NN = ((1,), (0,))


def split2(x):
    hi = x.astype(BF16)
    return hi, (x - hi.astype(F32)).astype(BF16)


def split3(x):
    hi = x.astype(BF16)
    rest = x - hi.astype(F32)
    mid = rest.astype(BF16)
    return hi, mid, (rest - mid.astype(F32)).astype(BF16)


def forward_kernel(
    heads, block, scale, limit_ref, pair, bias_w, gpair, qcat, kcat, gcat, vcat,
    e_out, d_out, stat_out, lbase, dbase, rows_buf,
):
    step = pl.program_id(0)

    @pl.when(step == 0)
    def _():
        def head(h, carry):
            q0, q1, q2 = split3(qcat[h])
            k0, k1, k2 = split3(kcat[h])
            lbase[h] = dot(
                jnp.concatenate([q0, q0, q1, q0, q2, q1], 0),
                jnp.concatenate([k0, k1, k0, k2, k0, k1], 0),
                TN,
            )
            g0, g1 = split2(gcat[h])
            v0, v1 = split2(vcat[h])
            dbase[h] = dot(
                jnp.concatenate([g0, g0, g1], 0), jnp.concatenate([v0, v1, v0], 0), TN
            )
            return carry

        lax.fori_loop(0, heads, head, 0)

    for r in range(block):
        w = jnp.concatenate([bias_w[...], gpair[r]], 0)
        rows_buf[r] = dot(w, pair[r], NT)
    cols = pair.shape[1]
    rows = pl.ds(pl.multiple_of(step * block, block), block)
    valid = lax.broadcasted_iota(jnp.int32, (block, cols), 1) < limit_ref[0]
    lane = lax.broadcasted_iota(jnp.int32, (block, 128), 1)
    peaks = jnp.zeros((block, 128), F32)
    totals = jnp.ones((block, 128), F32)
    uppers = jnp.zeros((block, 128), F32)
    for h in range(heads):
        logit = lbase[h, rows, :] + scale * rows_buf[:, h, :]
        logit = jnp.where(valid, logit, F32(-1000000000.0))
        peak = jnp.max(logit, axis=1, keepdims=True)
        e = jnp.exp(logit - peak)
        d = dbase[h, rows, :] + rows_buf[:, PAD + h, :]
        e_out[h] = e
        d_out[h] = d
        peaks = jnp.where(lane == h, peak, peaks)
        totals = jnp.where(lane == h, jnp.sum(e, axis=1, keepdims=True), totals)
        uppers = jnp.where(lane == h, jnp.sum(e * d, axis=1, keepdims=True), uppers)
    stat_out[0] = peaks
    stat_out[1] = totals
    stat_out[2] = uppers


def backward_kernel(
    heads, block, nq, nv, vwidth, pair, e_in, d_in, stats, own, w_hi, w_lo, gpair, qcat, kcat,
    gcat, vcat, pg_out, key_out, query_out, w_out, rows_buf, att_all, dl_all,
):
    step = pl.program_id(0)
    rows = pl.ds(pl.multiple_of(step * block, block), block)

    @pl.when(step == 0)
    def _():
        rows_buf[...] = jnp.zeros_like(rows_buf)
        w_out[...] = jnp.zeros_like(w_out)

    peers = stats.shape[0]
    top = stats[0, 0]
    for c in range(1, peers):
        top = jnp.maximum(top, stats[c, 0])
    total = jnp.zeros_like(top)
    upper = jnp.zeros_like(top)
    for c in range(peers):
        f = jnp.exp(stats[c, 0] - top)
        total = total + stats[c, 1] * f
        upper = upper + stats[c, 2] * f
    factor = jnp.exp(own[0] - top) / total
    delta = upper / total
    for h in range(heads):
        att = e_in[h] * factor[:, h : h + 1]
        dl = att * (d_in[h] - delta[:, h : h + 1])
        att_all[h, rows, :] = att
        dl_all[h, rows, :] = dl
        rows_buf[:, h, :] = dl
        rows_buf[:, PAD + h, :] = att
    acc = w_out[...]
    for r in range(block):
        a = rows_buf[r].astype(BF16)
        lhs = jnp.concatenate([a, a[:PAD]], 0)
        rhs = jnp.concatenate([w_hi[...], gpair[r], w_lo[...]], 0)
        pg_out[r] = dot(lhs, rhs, TN).astype(BF16)
        acc = acc + dot(a[:PAD], pair[r], NN)
    w_out[...] = acc

    @pl.when(step == pl.num_programs(0) - 1)
    def _():
        def head(h, carry):
            d0, d1 = split2(dl_all[h])
            a0, a1 = split2(att_all[h])
            q = jnp.concatenate(split2(qcat[h]), 0)
            k = jnp.concatenate(split2(kcat[h]), 0)
            g = jnp.concatenate(split2(gcat[h]), 0)
            v = jnp.concatenate(split2(vcat[h]), 0)
            kk = dot(q, d0, NN) + dot(q, d1, NN)
            key_out[h, :nq, :] = kk[:nq] + kk[nq:]
            vv = dot(g, a0, NN) + dot(g, a1, NN)
            half = g.shape[0] // 2
            key_out[h, nq:, :] = vv[:nv] + vv[half : half + nv]
            qq = dot(k, d0, NT) + dot(k, d1, NT)
            query_out[h, :nq, :] = qq[:nq] + qq[nq:]
            oo = dot(v, a0, NT) + dot(v, a1, NT)
            query_out[h, nq:, :] = oo[vwidth:nv] + oo[half + vwidth : half + nv]
            return carry

        lax.fori_loop(0, heads, head, 0)


def turn(rotation, local):
    return jnp.sum(rotation[:, :, None, :] * local[None], axis=1)


def turn_back(rotation, vector):
    return jnp.sum(rotation[:, :, None, :] * vector[:, None], axis=0)


def frame_terms(grad_global, local):
    rotation_part = jnp.sum(grad_global[:, None] * local[None], axis=2)
    return jnp.concatenate([rotation_part, jnp.sum(grad_global, axis=1)[:, None, :]], axis=1)


def by_head(x, heads):
    points = x.shape[1] // heads
    return x.reshape(3, heads, points, -1).transpose(1, 0, 2, 3).reshape(heads, 3 * points, -1)


def by_axis(x):
    heads, rows, m = x.shape
    return x.reshape(heads, 3, rows // 3, m).transpose(1, 0, 2, 3).reshape(3, heads * rows // 3, m)


def pad_rows(x, rows):
    return jnp.pad(x, ((0, 0), (0, rows - x.shape[1]), (0, 0)))


def per_device(
    pair_rep, bias_weight, head_weight, queries, key_vectors, values, query_points, key_points,
    value_points, rotations, translations, residue_count, grad_output, grad_points, grad_pair,
):
    channels, heads = bias_weight.shape
    width = queries.shape[0] // heads
    qpoints = query_points.shape[1] // heads
    vpoints = value_points.shape[1] // heads
    n_rows = queries.shape[1]
    n_cols = key_vectors.shape[1]
    logit_scale = math.sqrt(1.0 / 3.0)
    point_scale = math.sqrt(2.0 / (9.0 * qpoints))
    inner_scale = 1.0 / math.sqrt(width)
    coef = 0.5 * logit_scale * point_scale * jax.nn.softplus(head_weight)
    row_start = lax.axis_index("row") * n_rows
    col_start = lax.axis_index("col") * n_cols
    rot_rows = lax.dynamic_slice_in_dim(rotations, row_start, n_rows, 2)
    shift_rows = lax.dynamic_slice_in_dim(translations, row_start, n_rows, 1)
    rot_cols = lax.dynamic_slice_in_dim(rotations, col_start, n_cols, 2)
    shift_cols = lax.dynamic_slice_in_dim(translations, col_start, n_cols, 1)
    qg = by_head(turn(rot_rows, query_points) + shift_rows[:, None, :], heads)
    kg = by_head(turn(rot_cols, key_points) + shift_cols[:, None, :], heads)
    vg = by_head(turn(rot_cols, value_points) + shift_cols[:, None, :], heads)
    grad_flat = turn(rot_rows, grad_points)
    gg = by_head(grad_flat, heads)
    q = queries.reshape(heads, width, n_rows)
    k = key_vectors.reshape(heads, width, n_cols)
    qsize = width + 3 * qpoints
    nq = -(-(qsize + 2) // 16) * 16
    nv = width + 3 * vpoints
    nvp = -(-nv // 16) * 16
    c3 = coef[:, None, None]
    q_square = jnp.sum(qg * qg, axis=1, keepdims=True)
    k_square = jnp.sum(kg * kg, axis=1, keepdims=True)
    qcat = pad_rows(
        jnp.concatenate(
            [
                logit_scale * inner_scale * q,
                2.0 * c3 * qg,
                jnp.broadcast_to(-c3, (heads, 1, n_rows)),
                -c3 * q_square,
            ],
            axis=1,
        ),
        nq,
    )
    kcat = pad_rows(
        jnp.concatenate([k, kg, k_square, jnp.ones((heads, 1, n_cols), F32)], axis=1), nq
    )
    gcat = pad_rows(
        jnp.concatenate([grad_output.reshape(heads, width, n_rows), gg], axis=1), nvp
    )
    vcat = pad_rows(jnp.concatenate([values.reshape(heads, width, n_cols), vg], axis=1), nvp)
    w_t = jnp.pad(bias_weight.T, ((0, PAD - heads), (0, 0)))
    scaled = logit_scale * w_t.astype(F32)
    w_hi, w_lo = split2(scaled)
    gpair = pad_rows(grad_pair, PAD)
    limit = residue_count - col_start

    block = 8
    grid = (n_rows // block,)
    whole = lambda *shape: pl.BlockSpec(shape, lambda i: (0,) * len(shape))
    pair_spec = pl.BlockSpec((block, n_cols, channels), lambda i: (i, 0, 0))
    gpair_spec = pl.BlockSpec((block, PAD, channels), lambda i: (i, 0, 0))
    hij_spec = pl.BlockSpec((heads, block, n_cols), lambda i: (0, i, 0))
    stat_spec = pl.BlockSpec((3, block, 128), lambda i: (0, i, 0))
    cat_specs = [
        whole(heads, nq, n_rows),
        whole(heads, nq, n_cols),
        whole(heads, nvp, n_rows),
        whole(heads, nvp, n_cols),
    ]
    params = pltpu.CompilerParams(
        dimension_semantics=("arbitrary",), vmem_limit_bytes=VMEM_LIMIT
    )
    hij = jax.ShapeDtypeStruct((heads, n_rows, n_cols), F32)
    e_all, d_all, own = pl.pallas_call(
        functools.partial(forward_kernel, heads, block, logit_scale),
        grid=grid,
        in_specs=[
            pl.BlockSpec(memory_space=pltpu.SMEM),
            pair_spec,
            whole(PAD, channels),
            gpair_spec,
            *cat_specs,
        ],
        out_specs=[hij_spec, hij_spec, stat_spec],
        out_shape=[hij, hij, jax.ShapeDtypeStruct((3, n_rows, 128), F32)],
        scratch_shapes=[
            pltpu.VMEM((heads, n_rows, n_cols), F32),
            pltpu.VMEM((heads, n_rows, n_cols), F32),
            pltpu.VMEM((block, 2 * PAD, n_cols), F32),
        ],
        compiler_params=params,
    )(limit, pair_rep, w_t, gpair, qcat, kcat, gcat, vcat)

    stats = lax.all_gather(own, "col")
    peers = stats.shape[0]
    nk = nq + nv
    nr = nq + nv - width
    pair_grad, key_out, query_out, w_out = pl.pallas_call(
        functools.partial(backward_kernel, heads, block, nq, nv, width),
        grid=grid,
        in_specs=[
            pair_spec,
            hij_spec,
            hij_spec,
            pl.BlockSpec((peers, 3, block, 128), lambda i: (0, 0, i, 0)),
            stat_spec,
            whole(PAD, channels),
            whole(PAD, channels),
            gpair_spec,
            *cat_specs,
        ],
        out_specs=[
            pair_spec,
            whole(heads, nk, n_cols),
            whole(heads, nr, n_rows),
            whole(PAD, channels),
        ],
        out_shape=[
            jax.ShapeDtypeStruct(pair_rep.shape, BF16),
            jax.ShapeDtypeStruct((heads, nk, n_cols), F32),
            jax.ShapeDtypeStruct((heads, nr, n_rows), F32),
            jax.ShapeDtypeStruct((PAD, channels), F32),
        ],
        scratch_shapes=[
            pltpu.VMEM((block, 2 * PAD, n_cols), F32),
            pltpu.VMEM((heads, n_rows, n_cols), F32),
            pltpu.VMEM((heads, n_rows, n_cols), F32),
        ],
        compiler_params=params,
    )(pair_rep, e_all, d_all, stats, own, w_hi, w_lo, gpair, qcat, kcat, gcat, vcat)

    distance_part = jnp.sum(
        q_square[:, 0] * query_out[:, qsize + 1] + query_out[:, qsize], axis=1
    ) - 2.0 * jnp.sum(qg * query_out[:, width:qsize], axis=(1, 2))
    weight_part = logit_scale * w_out[:heads].T
    small = jnp.concatenate([weight_part.reshape(-1), distance_part])

    key_sum = lax.psum_scatter(
        key_out.reshape(heads * nk, n_cols), "row", scatter_dimension=1, tiled=True
    ).reshape(heads, nk, -1)
    query_sum = lax.psum_scatter(
        query_out.reshape(heads * nr, n_rows), "col", scatter_dimension=1, tiled=True
    ).reshape(heads, nr, -1)
    small = lax.psum(small, ("row", "col"))
    weight_total = small[: channels * heads].reshape(channels, heads)
    head_weight_grad = (
        small[channels * heads :]
        * (-0.5 * logit_scale * point_scale)
        * jax.nn.sigmoid(head_weight)
    )

    share = query_sum.shape[2]
    start = lax.axis_index("col") * share
    own_rows = lambda x: lax.dynamic_slice_in_dim(x, start, share, x.ndim - 1)
    rot_own = own_rows(rot_rows)
    shift_own = own_rows(shift_rows)
    query_grad = (logit_scale * inner_scale * query_sum[:, :width]).reshape(heads * width, share)
    dqg = by_axis(
        -2.0 * c3 * (own_rows(qg) * query_sum[:, qsize + 1][:, None] - query_sum[:, width:qsize])
    )
    point_out = by_axis(query_sum[:, nq:])
    query_point_grad = turn_back(rot_own, dqg)
    cotan_own = own_rows(grad_points)
    out_part = jnp.sum((point_out - shift_own[:, None, :])[:, None] * cotan_own[None], axis=2)
    out_part = jnp.concatenate(
        [out_part, -jnp.sum(own_rows(grad_flat), axis=1)[:, None, :]], axis=1
    )
    query_frame_grad = frame_terms(dqg, own_rows(query_points)) + out_part

    kshare = key_sum.shape[2]
    kstart = lax.axis_index("row") * kshare
    own_cols = lambda x: lax.dynamic_slice_in_dim(x, kstart, kshare, x.ndim - 1)
    rot_keys = own_cols(rot_cols)
    key_grad = key_sum[:, :width].reshape(heads * width, kshare)
    value_grad = key_sum[:, nq : nq + width].reshape(heads * width, kshare)
    dkg = by_axis(
        key_sum[:, width:qsize] + 2.0 * own_cols(kg) * key_sum[:, qsize][:, None]
    )
    dvg = by_axis(key_sum[:, nq + width :])
    key_point_grad = turn_back(rot_keys, dkg)
    value_point_grad = turn_back(rot_keys, dvg)
    key_frame_grad = frame_terms(dkg, own_cols(key_points)) + frame_terms(
        dvg, own_cols(value_points)
    )
    return (
        pair_grad, query_grad, query_point_grad, query_frame_grad, key_grad, value_grad,
        key_point_grad, value_point_grad, key_frame_grad, weight_total, head_weight_grad,
    )


def solution(mesh):
    return jax.shard_map(
        per_device,
        mesh=mesh,
        in_specs=(
            P("row", "col", None),
            P(),
            P(),
            P(None, "row"),
            P(None, "col"),
            P(None, "col"),
            P(None, None, "row"),
            P(None, None, "col"),
            P(None, None, "col"),
            P(),
            P(),
            P(),
            P(None, "row"),
            P(None, None, "row"),
            P("row", None, None),
        ),
        out_specs=(
            P("row", "col", None),
            P(None, ("row", "col")),
            P(None, None, ("row", "col")),
            P(None, None, ("row", "col")),
            P(None, ("col", "row")),
            P(None, ("col", "row")),
            P(None, None, ("col", "row")),
            P(None, None, ("col", "row")),
            P(None, None, ("col", "row")),
            P(),
            P(),
        ),
        check_vma=False,
    )
```

```python
import functools
import math

import jax
import jax.numpy as jnp
from jax import lax
from jax.experimental import pallas as pl
from jax.experimental.pallas import tpu as pltpu
from jax.sharding import PartitionSpec as P

F32 = jnp.float32
BF16 = jnp.bfloat16
PAD = 16
VMEM_LIMIT = 60 * 1024 * 1024


def dot(a, b, dims):
    return lax.dot_general(a, b, (dims, ((), ())), preferred_element_type=F32)


TN = ((0,), (0,))
NT = ((1,), (1,))
NN = ((1,), (0,))


def split2(x):
    hi = x.astype(BF16)
    return hi, (x - hi.astype(F32)).astype(BF16)


def split3(x):
    hi = x.astype(BF16)
    rest = x - hi.astype(F32)
    mid = rest.astype(BF16)
    return hi, mid, (rest - mid.astype(F32)).astype(BF16)


def forward_kernel(
    heads, block, scale, limit_ref, pair, bias_w, gpair, qcat, kcat, gcat, vcat,
    e_out, d_out, stat_out, lbase, dbase, rows_buf,
):
    step = pl.program_id(0)

    @pl.when(step == 0)
    def _():
        def head(h, carry):
            q0, q1, q2 = split3(qcat[h])
            k0, k1, k2 = split3(kcat[h])
            lbase[h] = dot(
                jnp.concatenate([q0, q0, q1, q0, q2, q1], 0),
                jnp.concatenate([k0, k1, k0, k2, k0, k1], 0),
                TN,
            )
            g0, g1 = split2(gcat[h])
            v0, v1 = split2(vcat[h])
            dbase[h] = dot(
                jnp.concatenate([g0, g0, g1], 0), jnp.concatenate([v0, v1, v0], 0), TN
            )
            return carry

        lax.fori_loop(0, heads, head, 0)

    for r in range(block):
        w = jnp.concatenate([bias_w[...], gpair[r]], 0)
        rows_buf[r] = dot(w, pair[r], NT)
    cols = pair.shape[1]
    rows = pl.ds(pl.multiple_of(step * block, block), block)
    valid = lax.broadcasted_iota(jnp.int32, (block, cols), 1) < limit_ref[0]
    lane = lax.broadcasted_iota(jnp.int32, (block, 128), 1)
    packed = jnp.ones((block, 128), F32)
    for h in range(heads):
        logit = lbase[h, rows, :] + scale * rows_buf[:, h, :]
        logit = jnp.where(valid, logit, F32(-1000000000.0))
        peak = jnp.max(logit, axis=1, keepdims=True)
        e = jnp.exp(logit - peak)
        d = dbase[h, rows, :] + rows_buf[:, PAD + h, :]
        e_out[h] = e
        d_out[h] = d
        packed = jnp.where(lane == h, peak, packed)
        packed = jnp.where(lane == PAD + h, jnp.sum(e, axis=1, keepdims=True), packed)
        packed = jnp.where(lane == 2 * PAD + h, jnp.sum(e * d, axis=1, keepdims=True), packed)
    stat_out[...] = packed


def merged(stats, own):
    peers = stats.shape[0]
    top = stats[0]
    for c in range(1, peers):
        top = jnp.maximum(top, stats[c])
    total = jnp.zeros_like(top)
    upper = jnp.zeros_like(top)
    for c in range(peers):
        f = jnp.exp(stats[c] - top)
        total = total + pltpu.roll(stats[c], 128 - PAD, 1) * f
        upper = upper + pltpu.roll(stats[c], 128 - 2 * PAD, 1) * f
    return jnp.exp(own - top) / total, upper / total


def sums_kernel(
    nq, nv, vwidth, e_in, d_in, stats, own, qcat, kcat, gcat, vcat, key_out, query_out
):
    h = pl.program_id(0)
    factor, delta = merged(stats, own[...])
    mine = lax.broadcasted_iota(jnp.int32, factor.shape, 1) == h
    pick = lambda x: jnp.sum(jnp.where(mine, x, 0.0), axis=1, keepdims=True)
    att = e_in[0] * pick(factor)
    dl = att * (d_in[0] - pick(delta))
    a0, a1 = split2(att)
    d0, d1 = split2(dl)
    q = jnp.concatenate(split2(qcat[0]), 0)
    k = jnp.concatenate(split2(kcat[0]), 0)
    g = jnp.concatenate(split2(gcat[0]), 0)
    v = jnp.concatenate(split2(vcat[0]), 0)
    kk = dot(q, d0, NN) + dot(q, d1, NN)
    key_out[0, :nq, :] = kk[:nq] + kk[nq:]
    vv = dot(g, a0, NN) + dot(g, a1, NN)
    half = g.shape[0] // 2
    key_out[0, nq:, :] = vv[:nv] + vv[half : half + nv]
    qq = dot(k, d0, NT) + dot(k, d1, NT)
    query_out[0, :nq, :] = qq[:nq] + qq[nq:]
    oo = dot(v, a0, NT) + dot(v, a1, NT)
    query_out[0, nq:, :] = oo[vwidth:nv] + oo[half + vwidth : half + nv]


def pair_kernel(
    heads, block, pair, e_in, d_in, stats, own, scaled, gpair, pg_out, w_out, rows_buf
):
    @pl.when(pl.program_id(0) == 0)
    def _():
        rows_buf[...] = jnp.zeros_like(rows_buf)
        w_out[...] = jnp.zeros_like(w_out)

    factor, delta = merged(stats, own[...])
    w_hi, w_lo = split2(scaled[...])
    for h in range(heads):
        att = e_in[h] * factor[:, h : h + 1]
        rows_buf[:, h, :] = att * (d_in[h] - delta[:, h : h + 1])
        rows_buf[:, PAD + h, :] = att
    acc = w_out[...]
    for r in range(block):
        a = rows_buf[r].astype(BF16)
        lhs = jnp.concatenate([a, a[:PAD]], 0)
        rhs = jnp.concatenate([w_hi, gpair[r], w_lo], 0)
        pg_out[r] = dot(lhs, rhs, TN).astype(BF16)
        acc = acc + dot(a[:PAD], pair[r], NN)
    w_out[...] = acc


def push_kernel(axes, sizes, total, x, out, slots, send, recv):
    count = math.prod(sizes)
    place = 0
    for axis, size in zip(axes, sizes):
        place = place * size + lax.axis_index(axis)
    copies = []
    for step in range(1, count):
        peer = lax.rem(place + step, count)
        device = {}
        rest = peer
        for axis, size in reversed(list(zip(axes, sizes))):
            device[axis] = lax.rem(rest, size)
            rest = rest // size
        copy = pltpu.make_async_remote_copy(
            src_ref=x,
            dst_ref=slots.at[place],
            send_sem=send.at[step],
            recv_sem=recv.at[place],
            device_id=device,
            device_id_type=pl.DeviceIdType.MESH,
        )
        copy.start()
        copies.append(copy)
    slots[place] = x[...]
    for step in range(1, count):
        source = lax.rem(place + step, count)
        pltpu.make_async_remote_copy(
            src_ref=x,
            dst_ref=slots.at[source],
            send_sem=send.at[step],
            recv_sem=recv.at[source],
            device_id=device,
            device_id_type=pl.DeviceIdType.MESH,
        ).wait_recv()
    for copy in copies:
        copy.wait_send()
    if total:
        acc = slots[0]
        for c in range(1, count):
            acc = acc + slots[c]
        out[...] = acc
    else:
        out[...] = slots[...]


def pushed(x, axes, total):
    sizes = tuple(lax.axis_size(axis) for axis in axes)
    count = math.prod(sizes)
    return pl.pallas_call(
        functools.partial(push_kernel, axes, sizes, total),
        in_specs=[pl.BlockSpec(memory_space=pltpu.VMEM)],
        out_specs=pl.BlockSpec(memory_space=pltpu.VMEM),
        out_shape=jax.ShapeDtypeStruct(x.shape if total else (count, *x.shape), F32),
        scratch_shapes=[
            pltpu.VMEM((count, *x.shape), F32),
            pltpu.SemaphoreType.DMA((count,)),
            pltpu.SemaphoreType.DMA((count,)),
        ],
        compiler_params=pltpu.CompilerParams(has_side_effects=True),
    )(x)


def turn(rotation, local):
    return jnp.sum(rotation[:, :, None, :] * local[None], axis=1)


def turn_back(rotation, vector):
    return jnp.sum(rotation[:, :, None, :] * vector[:, None], axis=0)


def frame_terms(grad_global, local):
    rotation_part = jnp.sum(grad_global[:, None] * local[None], axis=2)
    return jnp.concatenate([rotation_part, jnp.sum(grad_global, axis=1)[:, None, :]], axis=1)


def by_head(x, heads):
    points = x.shape[1] // heads
    return x.reshape(3, heads, points, -1).transpose(1, 0, 2, 3).reshape(heads, 3 * points, -1)


def by_axis(x):
    heads, rows, m = x.shape
    return x.reshape(heads, 3, rows // 3, m).transpose(1, 0, 2, 3).reshape(3, heads * rows // 3, m)


def pad_rows(x, rows):
    return jnp.pad(x, ((0, 0), (0, rows - x.shape[1]), (0, 0)))


def per_device(
    pair_rep, bias_weight, head_weight, queries, key_vectors, values, query_points, key_points,
    value_points, rotations, translations, residue_count, grad_output, grad_points, grad_pair,
):
    channels, heads = bias_weight.shape
    width = queries.shape[0] // heads
    qpoints = query_points.shape[1] // heads
    vpoints = value_points.shape[1] // heads
    n_rows = queries.shape[1]
    n_cols = key_vectors.shape[1]
    logit_scale = math.sqrt(1.0 / 3.0)
    point_scale = math.sqrt(2.0 / (9.0 * qpoints))
    inner_scale = 1.0 / math.sqrt(width)
    coef = 0.5 * logit_scale * point_scale * jax.nn.softplus(head_weight)
    row_start = lax.axis_index("row") * n_rows
    col_start = lax.axis_index("col") * n_cols
    rot_rows = lax.dynamic_slice_in_dim(rotations, row_start, n_rows, 2)
    shift_rows = lax.dynamic_slice_in_dim(translations, row_start, n_rows, 1)
    rot_cols = lax.dynamic_slice_in_dim(rotations, col_start, n_cols, 2)
    shift_cols = lax.dynamic_slice_in_dim(translations, col_start, n_cols, 1)
    qg = by_head(turn(rot_rows, query_points) + shift_rows[:, None, :], heads)
    kg = by_head(turn(rot_cols, key_points) + shift_cols[:, None, :], heads)
    vg = by_head(turn(rot_cols, value_points) + shift_cols[:, None, :], heads)
    grad_flat = turn(rot_rows, grad_points)
    gg = by_head(grad_flat, heads)
    q = queries.reshape(heads, width, n_rows)
    k = key_vectors.reshape(heads, width, n_cols)
    qsize = width + 3 * qpoints
    nq = -(-(qsize + 2) // 16) * 16
    nv = width + 3 * vpoints
    nvp = -(-nv // 16) * 16
    c3 = coef[:, None, None]
    q_square = jnp.sum(qg * qg, axis=1, keepdims=True)
    k_square = jnp.sum(kg * kg, axis=1, keepdims=True)
    qcat = pad_rows(
        jnp.concatenate(
            [
                logit_scale * inner_scale * q,
                2.0 * c3 * qg,
                jnp.broadcast_to(-c3, (heads, 1, n_rows)),
                -c3 * q_square,
            ],
            axis=1,
        ),
        nq,
    )
    kcat = pad_rows(
        jnp.concatenate([k, kg, k_square, jnp.ones((heads, 1, n_cols), F32)], axis=1), nq
    )
    gcat = pad_rows(
        jnp.concatenate([grad_output.reshape(heads, width, n_rows), gg], axis=1), nvp
    )
    vcat = pad_rows(jnp.concatenate([values.reshape(heads, width, n_cols), vg], axis=1), nvp)
    w_t = jnp.pad(bias_weight.T, ((0, PAD - heads), (0, 0)))
    scaled = logit_scale * w_t.astype(F32)
    gpair = pad_rows(grad_pair, PAD)
    limit = residue_count - col_start

    block = 8
    grid = (n_rows // block,)
    whole = lambda *shape: pl.BlockSpec(shape, lambda i: (0,) * len(shape))
    pair_spec = pl.BlockSpec((block, n_cols, channels), lambda i: (i, 0, 0))
    gpair_spec = pl.BlockSpec((block, PAD, channels), lambda i: (i, 0, 0))
    hij_spec = pl.BlockSpec((heads, block, n_cols), lambda i: (0, i, 0))
    stat_spec = pl.BlockSpec((block, 128), lambda i: (i, 0))
    cat_specs = [
        whole(heads, nq, n_rows),
        whole(heads, nq, n_cols),
        whole(heads, nvp, n_rows),
        whole(heads, nvp, n_cols),
    ]
    params = pltpu.CompilerParams(
        dimension_semantics=("arbitrary",), vmem_limit_bytes=VMEM_LIMIT
    )
    hij = jax.ShapeDtypeStruct((heads, n_rows, n_cols), F32)
    e_all, d_all, own = pl.pallas_call(
        functools.partial(forward_kernel, heads, block, logit_scale),
        grid=grid,
        in_specs=[
            pl.BlockSpec(memory_space=pltpu.SMEM),
            pair_spec,
            whole(PAD, channels),
            gpair_spec,
            *cat_specs,
        ],
        out_specs=[hij_spec, hij_spec, stat_spec],
        out_shape=[hij, hij, jax.ShapeDtypeStruct((n_rows, 128), F32)],
        scratch_shapes=[
            pltpu.VMEM((heads, n_rows, n_cols), F32),
            pltpu.VMEM((heads, n_rows, n_cols), F32),
            pltpu.VMEM((block, 2 * PAD, n_cols), F32),
        ],
        compiler_params=params,
    )(limit, pair_rep, w_t, gpair, qcat, kcat, gcat, vcat)

    stats = pushed(own, ("col",), False)
    peers = stats.shape[0]
    nk = nq + nv
    nr = nq + nv - width
    per_head = lambda *shape: pl.BlockSpec((1, *shape), lambda i: (i, 0, 0))
    key_out, query_out = pl.pallas_call(
        functools.partial(sums_kernel, nq, nv, width),
        grid=(heads,),
        in_specs=[
            per_head(n_rows, n_cols),
            per_head(n_rows, n_cols),
            whole(peers, n_rows, 128),
            whole(n_rows, 128),
            per_head(nq, n_rows),
            per_head(nq, n_cols),
            per_head(nvp, n_rows),
            per_head(nvp, n_cols),
        ],
        out_specs=[per_head(nk, n_cols), per_head(nr, n_rows)],
        out_shape=[
            jax.ShapeDtypeStruct((heads, nk, n_cols), F32),
            jax.ShapeDtypeStruct((heads, nr, n_rows), F32),
        ],
        compiler_params=params,
    )(e_all, d_all, stats, own, qcat, kcat, gcat, vcat)
    key_sum = lax.psum_scatter(
        key_out.reshape(heads * nk, n_cols), "row", scatter_dimension=1, tiled=True
    ).reshape(heads, nk, -1)
    query_sum = lax.psum_scatter(
        query_out.reshape(heads * nr, n_rows), "col", scatter_dimension=1, tiled=True
    ).reshape(heads, nr, -1)
    pair_grad, w_out = pl.pallas_call(
        functools.partial(pair_kernel, heads, block),
        grid=grid,
        in_specs=[
            pair_spec,
            hij_spec,
            hij_spec,
            pl.BlockSpec((peers, block, 128), lambda i: (0, i, 0)),
            stat_spec,
            whole(PAD, channels),
            gpair_spec,
        ],
        out_specs=[pair_spec, whole(PAD, channels)],
        out_shape=[
            jax.ShapeDtypeStruct(pair_rep.shape, BF16),
            jax.ShapeDtypeStruct((PAD, channels), F32),
        ],
        scratch_shapes=[pltpu.VMEM((block, 2 * PAD, n_cols), F32)],
        compiler_params=params,
        cost_estimate=pl.CostEstimate(
            flops=8 * n_rows * n_cols * channels * PAD,
            bytes_accessed=4 * n_rows * n_cols * channels + 8 * heads * n_rows * n_cols,
            transcendentals=0,
        ),
    )(pair_rep, e_all, d_all, stats, own, scaled, gpair)

    distance_part = jnp.sum(
        q_square[:, 0] * query_out[:, qsize + 1] + query_out[:, qsize], axis=1
    ) - 2.0 * jnp.sum(qg * query_out[:, width:qsize], axis=(1, 2))
    small = jnp.concatenate(
        [logit_scale * w_out, jnp.pad(distance_part, (0, 8 * channels - heads)).reshape(8, channels)]
    )
    small = pushed(small, ("row", "col"), True)
    weight_total = small[:heads].T
    head_weight_grad = (
        small[PAD, :heads] * (-0.5 * logit_scale * point_scale) * jax.nn.sigmoid(head_weight)
    )

    share = query_sum.shape[2]
    start = lax.axis_index("col") * share
    own_rows = lambda x: lax.dynamic_slice_in_dim(x, start, share, x.ndim - 1)
    rot_own = own_rows(rot_rows)
    shift_own = own_rows(shift_rows)
    query_grad = (logit_scale * inner_scale * query_sum[:, :width]).reshape(heads * width, share)
    dqg = by_axis(
        -2.0 * c3 * (own_rows(qg) * query_sum[:, qsize + 1][:, None] - query_sum[:, width:qsize])
    )
    point_out = by_axis(query_sum[:, nq:])
    query_point_grad = turn_back(rot_own, dqg)
    cotan_own = own_rows(grad_points)
    out_part = jnp.sum((point_out - shift_own[:, None, :])[:, None] * cotan_own[None], axis=2)
    out_part = jnp.concatenate(
        [out_part, -jnp.sum(own_rows(grad_flat), axis=1)[:, None, :]], axis=1
    )
    query_frame_grad = frame_terms(dqg, own_rows(query_points)) + out_part

    kshare = key_sum.shape[2]
    kstart = lax.axis_index("row") * kshare
    own_cols = lambda x: lax.dynamic_slice_in_dim(x, kstart, kshare, x.ndim - 1)
    rot_keys = own_cols(rot_cols)
    key_grad = key_sum[:, :width].reshape(heads * width, kshare)
    value_grad = key_sum[:, nq : nq + width].reshape(heads * width, kshare)
    dkg = by_axis(
        key_sum[:, width:qsize] + 2.0 * own_cols(kg) * key_sum[:, qsize][:, None]
    )
    dvg = by_axis(key_sum[:, nq + width :])
    key_point_grad = turn_back(rot_keys, dkg)
    value_point_grad = turn_back(rot_keys, dvg)
    key_frame_grad = frame_terms(dkg, own_cols(key_points)) + frame_terms(
        dvg, own_cols(value_points)
    )
    return (
        pair_grad, query_grad, query_point_grad, query_frame_grad, key_grad, value_grad,
        key_point_grad, value_point_grad, key_frame_grad, weight_total, head_weight_grad,
    )


def solution(mesh):
    return jax.shard_map(
        per_device,
        mesh=mesh,
        in_specs=(
            P("row", "col", None),
            P(),
            P(),
            P(None, "row"),
            P(None, "col"),
            P(None, "col"),
            P(None, None, "row"),
            P(None, None, "col"),
            P(None, None, "col"),
            P(),
            P(),
            P(),
            P(None, "row"),
            P(None, None, "row"),
            P("row", None, None),
        ),
        out_specs=(
            P("row", "col", None),
            P(None, ("row", "col")),
            P(None, None, ("row", "col")),
            P(None, None, ("row", "col")),
            P(None, ("col", "row")),
            P(None, ("col", "row")),
            P(None, None, ("col", "row")),
            P(None, None, ("col", "row")),
            P(None, None, ("col", "row")),
            P(),
            P(),
        ),
        check_vma=False,
    )
```
